16 devices in a mesh: dp: 2 (over y, z), tp: 8 (over x, core).
Axes of the slice: x: 4, y: 2, z: 1, core: 2. Of those that a mesh axis runs over, the one named last changes fastest.
The devices are a block of a 4x4x8 slice.
Arguments:
- x: bfloat16 [4096, 5120], P('dp'), parts along dimension 0
- w_gate: bfloat16 [5120, 27648], P(None, 'tp')
- w_up: bfloat16 [5120, 27648], P(None, 'tp')
- w_down: bfloat16 [27648, 5120], P('tp')
Outputs:
- output: bfloat16 [4096, 5120], P('dp'), parts along dimension 0
There are 2 independent parts. The reference program is written for one: setup_inputs(seed, part) draws one part's arguments, and reference() takes and returns one part's arrays. A program takes and returns all parts, laid end to end along the dimension named above; an argument that names none is the same for every part.
All inputs are finite; a program needn't handle non-finite values.
Results may differ from the reference program's by a relative error of at most 0.016.
Values are sent between devices in bfloat16 or wider.
A program may use at most 768 MiB of HBM per device.

```python
import jax
import jax.numpy as jnp

ROWS = 2048
D = 5120
FF = 27648


def setup_inputs(seed: int = 0, part: int = 0) -> dict:
    kx, kg, ku, kd = jax.random.split(jax.random.key(seed), 4)
    drawn = {
        "x": jax.random.normal(jax.random.fold_in(kx, part), (ROWS, D), jnp.float32),
        "w_gate": jax.random.normal(kg, (D, FF), jnp.float32) * D**-0.5,
        "w_up": jax.random.normal(ku, (D, FF), jnp.float32) * D**-0.5,
        "w_down": jax.random.normal(kd, (FF, D), jnp.float32) * FF**-0.5,
    }
    return {k: v.astype(jnp.bfloat16) for k, v in drawn.items()}


def reference(x, w_gate, w_up, w_down):
    gate = jnp.dot(x, w_gate, preferred_element_type=jnp.float32)
    up = jnp.dot(x, w_up, preferred_element_type=jnp.float32)
    hidden = (jax.nn.silu(gate) * up).astype(jnp.bfloat16)
    return jnp.dot(hidden, w_down, preferred_element_type=jnp.float32).astype(jnp.bfloat16)
```

```python
import functools

import jax
import jax.numpy as jnp
from jax import lax
from jax.experimental import pallas as pl
from jax.experimental.pallas import tpu as pltpu
from jax.sharding import PartitionSpec as P

BF16, F32 = jnp.bfloat16, jnp.float32
MESH = pl.DeviceIdType.MESH
CORES = 2
ROWS = 512
GU_COLS = 384
D_COLS = 512


def block(n, x, w_gate, w_up, w_down):
    rows, d = x.shape
    f = w_gate.shape[1]
    chips = n // CORES
    assert chips == 4
    half = d // CORES
    r_, gb, db = ROWS, GU_COLS, D_COLS
    nr, ng, nd = rows // r_, f // gb, half // db
    assert nr * r_ == rows and ng * gb == f and nd * db == half
    assert ng == 9 and nd == 5
    piece = r_ // chips
    hp = piece // 2

    def kernel(x_ref, wg_ref, wu_ref, wd_ref, y_ref, wdp_ref, xb, wgu, wdb, hid, sb, rly, dirb, relb,
               x_sem, g_sem, d_sem, wd_send, wd_recv, h_send, h_recv, credit,
               rly_send, rly_recv, dir_send, dir_recv, rel_send, rel_recv,
               ag_send, ag_recv, agp_send, fw_send, fw_recv, loc_sem, p_send, p_recv):
        me = lax.axis_index("tp")
        chip, core = me // CORES, lax.rem(me, CORES)
        right_chip, left_chip = lax.rem(chip + 1, chips), lax.rem(chip + chips - 1, chips)
        far_chip = lax.rem(chip + 2, chips)
        right, left = right_chip * CORES + core, left_chip * CORES + core
        partner = chip * CORES + (1 - core)
        sides = (right, left)
        my_half = core * half
        partner_half = (1 - core) * half

        def ds(start, size, m):
            return pl.ds(pl.multiple_of(start, m), size)

        def remote(src, dst, send, recv, to):
            return pltpu.make_async_remote_copy(
                src_ref=src, dst_ref=dst, send_sem=send, recv_sem=recv,
                device_id={"tp": to}, device_id_type=MESH)

        def x_copy(r):
            return pltpu.make_async_copy(x_ref.at[ds(r * r_, r_, r_)], xb, x_sem)

        def gu_copies(j, slot):
            cols = ds(j * gb, gb, 128)
            return (pltpu.make_async_copy(wg_ref.at[:, cols], wgu.at[slot, :, pl.ds(0, gb)], g_sem.at[slot, 0]),
                    pltpu.make_async_copy(wu_ref.at[:, cols], wgu.at[slot, :, pl.ds(gb, gb)], g_sem.at[slot, 1]))

        def d_copies(k, slot):
            return (pltpu.make_async_copy(wd_ref.at[:, ds(my_half + k * db, db, 128)], wdb.at[slot, pl.ds(0, f)], d_sem.at[slot, 0]),
                    pltpu.make_async_copy(wdp_ref.at[:, ds(k * db, db, 128)], wdb.at[slot, pl.ds(f, f)], d_sem.at[slot, 1]))

        def wd_copy(k):
            return remote(wd_ref.at[:, ds(partner_half + k * db, db, 128)], wdp_ref.at[:, ds(k * db, db, 128)],
                          wd_send.at[k], wd_recv.at[k], partner)

        def h_copy(j):
            return remote(hid.at[:, ds(j * gb, gb, 128)], hid.at[:, ds(f + j * gb, gb, 128)], h_send, h_recv, partner)

        def h_all():
            return remote(hid.at[:, pl.ds(0, f)], hid.at[:, pl.ds(f, f)], h_send, h_recv, partner)

        def rows_of(q, part):
            return ds(q * piece + part * hp, hp, hp)

        def rly_copy(k, s):
            return remote(sb.at[k, rows_of(far_chip, s)], rly.at[s, k], rly_send.at[s, k], rly_recv.at[s, k], sides[s])

        def dir_copy(k, s):
            to_chip = (right_chip, left_chip)[s]
            return remote(sb.at[k, rows_of(to_chip, 1 - s)], dirb.at[s, k], dir_send.at[s, k], dir_recv.at[s, k], sides[s])

        def rel_copy(k, s):
            to_chip = (right_chip, left_chip)[s]
            return remote(sb.at[k, rows_of(to_chip, s)], relb.at[s, k], rel_send.at[s, k], rel_recv.at[s, k], sides[s])

        def y_at(r, q, k, part=None):
            cols = ds(my_half + k * db, db, 128)
            if part is None:
                return y_ref.at[ds(r * r_ + q * piece, piece, piece), cols]
            return y_ref.at[ds(r * r_ + q * piece + part * hp, hp, hp), cols]

        def own_piece(k):
            return sb.at[k, ds(chip * piece, piece, piece)]

        def loc_copy(r, k):
            return pltpu.make_async_copy(own_piece(k), y_at(r, chip, k), loc_sem.at[k])

        def ag_copy(r, k, s):
            return remote(own_piece(k), y_at(r, chip, k), ag_send.at[s, k], ag_recv.at[s, k], sides[s])

        def agp_copy(r, k):
            return remote(own_piece(k), y_at(r, chip, k), agp_send.at[k], p_recv, partner)

        def fw_copy(r, k, s):
            q = (left_chip, right_chip)[s]
            return remote(y_at(r, q, k, s), y_at(r, q, k, s), fw_send.at[s, k], fw_recv.at[s, k], sides[s])

        def p_copy(r, k, q):
            return remote(y_at(r, q, k), y_at(r, q, k), p_send, p_recv, partner)

        def first_sends(k):
            for s in range(2):
                rly_copy(k, s).start()
            for s in range(2):
                dir_copy(k, s).start()

        def stage1(k):
            for s in range(2):
                rly_copy(k, s).wait_recv()
                rr = rows_of((right_chip, left_chip)[s], s)
                sb[k, rr] = (sb[k, rr].astype(F32) + rly[s, k].astype(F32)).astype(BF16)
            for s in range(2):
                rel_copy(k, s).start()

        def stage2(r, k):
            for s in range(2):
                rly_copy(k, s).wait_send()
                dir_copy(k, s).wait()
                rel_copy(k, s).wait_recv()
            for part in range(2):
                rr = rows_of(chip, part)
                from_left = (relb if part == 0 else dirb)[0, k].astype(F32)
                from_right = (relb if part == 1 else dirb)[1, k].astype(F32)
                sb[k, rr] = (sb[k, rr].astype(F32) + from_left + from_right).astype(BF16)
            for s in range(2):
                ag_copy(r, k, s).start()
            agp_copy(r, k).start()
            loc_copy(r, k).start()

        def stage3(r, k):
            for s in range(2):
                rel_copy(k, s).wait_send()
                ag_copy(r, k, s).wait_recv()
            for s in range(2):
                fw_copy(r, k, s).start()
            p_copy(r, k, left_chip).start()
            p_copy(r, k, right_chip).start()
            loc_copy(r, k).wait()

        def stage4(r, k):
            for s in range(2):
                ag_copy(r, k, s).wait_send()
                fw_copy(r, k, s).wait()
            agp_copy(r, k).wait_send()
            p_copy(r, k, far_chip).start()

        def events(j, r):
            @pl.when(j < 2)
            def _():
                stage1(j + 3)

            @pl.when(j < 4)
            def _():
                stage2(r, j + 1)

            @pl.when(jnp.logical_and(j >= 2, j < 7))
            def _():
                stage3(r, j - 2)

            @pl.when(j >= 4)
            def _():
                stage4(r, j - 4)

        x_copy(0).start()
        for j in range(2):
            for c in gu_copies(j, j):
                c.start()
        barrier = pltpu.get_barrier_semaphore()
        for to in (right, left, partner):
            pl.semaphore_signal(barrier, inc=1, device_id={"tp": to}, device_id_type=MESH)
        pl.semaphore_wait(barrier, 3)
        for k in range(nd):
            wd_copy(k).start()

        def start_down(r, k):
            @pl.when(r == 0)
            def _():
                wd_copy(k).wait_recv()
            for c in d_copies(k, lax.rem(k, 2)):
                c.start()

        def chunk(r, _):
            x_copy(r).wait()

            def gate_up(j, _):
                slot = lax.rem(r * ng + j, 2)
                for c in gu_copies(j, slot):
                    c.wait()

                @pl.when(r > 0)
                def _():
                    events(j, r - 1)
                acc = jnp.dot(xb[...], wgu[slot], preferred_element_type=F32)
                gate, up = acc[:, :gb], acc[:, gb:]
                hid[:, ds(j * gb, gb, 128)] = (jax.nn.silu(gate) * up).astype(BF16)

                @pl.when(jnp.logical_and(r > 0, j == 0))
                def _():
                    pl.semaphore_wait(credit, 1)

                @pl.when(jnp.logical_or(r < nr - 1, j < ng - 2))
                def _():
                    for c in gu_copies(lax.rem(j + 2, ng), slot):
                        c.start()
                h_copy(j).start()

                @pl.when(j == 3)
                def _():
                    start_down(r, 0)

                @pl.when(j == 5)
                def _():
                    start_down(r, 1)
                return 0

            lax.fori_loop(0, ng, gate_up, 0)

            @pl.when(r < nr - 1)
            def _():
                x_copy(r + 1).start()
            h_all().wait()

            def down(k, _):
                slot = lax.rem(k, 2)
                for c in d_copies(k, slot):
                    c.wait()
                acc = jnp.dot(hid[...], wdb[slot], preferred_element_type=F32)
                sb[k] = acc.astype(BF16)

                @pl.when(k < nd - 2)
                def _():
                    start_down(r, k + 2)
                first_sends(k)

                @pl.when(k >= 2)
                def _():
                    stage1(k - 2)

                @pl.when(k == nd - 1)
                def _():
                    stage2(r, 0)
                return 0

            lax.fori_loop(0, nd, down, 0)

            @pl.when(r < nr - 1)
            def _():
                pl.semaphore_signal(credit, inc=1, device_id={"tp": partner}, device_id_type=MESH)
            return 0

        lax.fori_loop(0, nr, chunk, 0)

        def tail(j, _):
            events(j, nr - 1)
            return 0

        lax.fori_loop(0, ng, tail, 0)
        for k in range(nd):
            wd_copy(k).wait_send()
        sent = y_ref.at[pl.ds(0, rows - rows // chips), ds(my_half, half, 128)]
        came = y_ref.at[:, ds(partner_half, half, 128)]
        remote(sent, sent, p_send, p_recv, partner).wait_send()
        remote(came, came, p_send, p_recv, partner).wait_recv()

    dma = pltpu.SemaphoreType.DMA
    y, _ = pl.pallas_call(
        kernel,
        out_shape=(jax.ShapeDtypeStruct((rows, d), BF16), jax.ShapeDtypeStruct((f, half), BF16)),
        in_specs=[pl.BlockSpec(memory_space=pl.ANY)] * 4,
        out_specs=(pl.BlockSpec(memory_space=pl.ANY),) * 2,
        scratch_shapes=[
            pltpu.VMEM((r_, d), BF16),
            pltpu.VMEM((2, d, 2 * gb), BF16),
            pltpu.VMEM((2, CORES * f, db), BF16),
            pltpu.VMEM((r_, CORES * f), BF16),
            pltpu.VMEM((nd, r_, db), BF16),
            pltpu.VMEM((2, nd, hp, db), BF16),
            pltpu.VMEM((2, nd, hp, db), BF16),
            pltpu.VMEM((2, nd, hp, db), BF16),
            dma, dma((2, 2)), dma((2, 2)),
            dma((nd,)), dma((nd,)), dma, dma, pltpu.SemaphoreType.REGULAR,
            dma((2, nd)), dma((2, nd)), dma((2, nd)), dma((2, nd)), dma((2, nd)), dma((2, nd)),
            dma((2, nd)), dma((2, nd)), dma((nd,)), dma((2, nd)), dma((2, nd)), dma((nd,)), dma, dma,
        ],
        compiler_params=pltpu.CompilerParams(
            collective_id=0, has_side_effects=True, vmem_limit_bytes=67043328),
        cost_estimate=pl.CostEstimate(flops=6 * rows * d * f, bytes_accessed=2 * 3 * d * f * nr, transcendentals=rows * f),
        name="mlp_block",
    )(x, w_gate, w_up, w_down)
    return y


def solution(mesh):
    return jax.shard_map(
        functools.partial(block, mesh.shape["tp"]),
        mesh=mesh,
        in_specs=(P("dp", None), P(None, "tp"), P(None, "tp"), P("tp", None)),
        out_specs=P("dp", None),
        check_vma=False,
    )
```

```python
import functools

import jax
import jax.numpy as jnp
from jax import lax
from jax.experimental import pallas as pl
from jax.experimental.pallas import tpu as pltpu
from jax.sharding import PartitionSpec as P

BF16, F32 = jnp.bfloat16, jnp.float32
MESH = pl.DeviceIdType.MESH
CORES = 2
CHUNKS = (4, 4, 4, 4)
KERNEL_VMEM = 42_500_000
GU_COLS = 384
D_COLS = 512


def join(d, *parts):
    sizes = [p.shape[0] for p in parts]
    starts = [sum(sizes[:i]) for i in range(len(parts))]

    def kernel(*refs):
        *ins, y_ref, sem = refs
        copies = [
            pltpu.make_async_copy(ref.at[:, pl.ds(0, d)], y_ref.at[pl.ds(start, n)], sem.at[i])
            for i, (ref, start, n) in enumerate(zip(ins, starts, sizes))
        ]
        for c in copies:
            c.start()
        for c in copies:
            c.wait()

    return pl.pallas_call(
        kernel,
        out_shape=jax.ShapeDtypeStruct((sum(sizes), d), BF16),
        in_specs=[pl.BlockSpec(memory_space=pltpu.VMEM)] * len(parts),
        out_specs=pl.BlockSpec(memory_space=pl.ANY),
        scratch_shapes=[pltpu.SemaphoreType.DMA((len(parts),))],
        compiler_params=pltpu.CompilerParams(vmem_limit_bytes=4_000_000),
        name="join",
    )(*parts)


def block(n, x, w_gate, w_up, w_down):
    rows, d = x.shape
    f = w_gate.shape[1]
    chips = n // CORES
    assert chips == 4
    half = d // CORES
    gb, db = GU_COLS, D_COLS
    nr, ng, nd = len(CHUNKS), f // gb, half // db
    unit = rows // sum(CHUNKS)
    size = [c * unit for c in CHUNKS]
    base = [sum(size[:r]) for r in range(nr)]
    top = max(size)
    assert sum(size) == rows and ng * gb == f and nd * db == half
    assert ng == 9 and nd == 5
    parts = 2 * chips
    assert all(c % (16 * parts) == 0 for c in size)
    assert size[0] == size[-1] == top

    def kernel(x_ref, wg_ref, wu_ref, wd_ref, hid, mid_ref, xb, early_ref, wdp_ref, wgu, wdb, sb, rly, dirb, relb,
               x_sem, g_sem, d_sem, wd_send, wd_recv, h_send, h_recv, credit,
               rly_send, rly_recv, dir_send, dir_recv, rel_send, rel_recv,
               ag_send, ag_recv, agp_send, fw_send, fw_recv, loc_sem, p_send, p_recv):
        me = lax.axis_index("tp")
        chip, core = me // CORES, lax.rem(me, CORES)
        right_chip, left_chip = lax.rem(chip + 1, chips), lax.rem(chip + chips - 1, chips)
        far_chip = lax.rem(chip + 2, chips)
        right, left = right_chip * CORES + core, left_chip * CORES + core
        partner = chip * CORES + (1 - core)
        sides = (right, left)
        my_half = core * half
        partner_half = (1 - core) * half

        def ds(start, size, m):
            return pl.ds(pl.multiple_of(start, m), size)

        def remote(src, dst, send, recv, to):
            return pltpu.make_async_remote_copy(
                src_ref=src, dst_ref=dst, send_sem=send, recv_sem=recv,
                device_id={"tp": to}, device_id_type=MESH)

        def x_copy(r):
            return pltpu.make_async_copy(x_ref.at[pl.ds(base[r], size[r])], xb.at[pl.ds(0, size[r])], x_sem)

        def gu_copies(j, slot):
            cols = ds(j * gb, gb, 128)
            return (pltpu.make_async_copy(wg_ref.at[:, cols], wgu.at[slot, :, pl.ds(0, gb)], g_sem.at[slot, 0]),
                    pltpu.make_async_copy(wu_ref.at[:, cols], wgu.at[slot, :, pl.ds(gb, gb)], g_sem.at[slot, 1]))

        def d_copies(k, slot):
            return (pltpu.make_async_copy(wd_ref.at[:, ds(my_half + k * db, db, 128)], wdb.at[slot, pl.ds(0, f)], d_sem.at[slot, 0]),
                    pltpu.make_async_copy(wdp_ref.at[:, ds(k * db, db, 128)], wdb.at[slot, pl.ds(f, f)], d_sem.at[slot, 1]))

        def wd_copy(k):
            return remote(wd_ref.at[:, ds(partner_half + k * db, db, 128)], wdp_ref.at[:, ds(k * db, db, 128)],
                          wd_send.at[k], wd_recv.at[k], partner)

        def h_copy(r, j):
            at = pl.ds(0, size[r])
            return remote(hid.at[at, ds(j * gb, gb, 128)], hid.at[at, ds(f + j * gb, gb, 128)], h_send, h_recv, partner)

        def h_all(r):
            at = pl.ds(0, size[r])
            return remote(hid.at[at, pl.ds(0, f)], hid.at[at, pl.ds(f, f)], h_send, h_recv, partner)

        def rows_of(r, q, part):
            hp = size[r] // parts
            return ds(q * 2 * hp + part * hp, hp, hp)

        def rly_copy(r, k, s):
            return remote(sb.at[k, rows_of(r, far_chip, s)], rly.at[s, k, pl.ds(0, size[r] // parts)], rly_send.at[s, k], rly_recv.at[s, k], sides[s])

        def dir_copy(r, k, s):
            to_chip = (right_chip, left_chip)[s]
            return remote(sb.at[k, rows_of(r, to_chip, 1 - s)], dirb.at[s, k, pl.ds(0, size[r] // parts)], dir_send.at[s, k], dir_recv.at[s, k], sides[s])

        def rel_copy(r, k, s):
            to_chip = (right_chip, left_chip)[s]
            return remote(sb.at[k, rows_of(r, to_chip, s)], relb.at[s, k, pl.ds(0, size[r] // parts)], rel_send.at[s, k], rel_recv.at[s, k], sides[s])

        def place(r):
            return (early_ref, 0) if r == 0 else (xb, 0) if r == nr - 1 else (mid_ref, base[r] - base[1])

        def group(r):
            return 0 if r == 0 else 2 if r == nr - 1 else 1

        def y_at(r, q, k, part=None):
            cols = ds(my_half + k * db, db, 128)
            hp = size[r] // parts
            ref, start = place(r)
            if part is None:
                return ref.at[ds(start + q * 2 * hp, 2 * hp, hp), cols]
            return ref.at[ds(start + q * 2 * hp + part * hp, hp, hp), cols]

        def own_piece(r, k):
            hp = size[r] // parts
            return sb.at[k, ds(chip * 2 * hp, 2 * hp, 2 * hp)]

        def loc_copy(r, k):
            return pltpu.make_async_copy(own_piece(r, k), y_at(r, chip, k), loc_sem.at[k])

        def ag_copy(r, k, s):
            return remote(own_piece(r, k), y_at(r, chip, k), ag_send.at[s, k], ag_recv.at[s, k], sides[s])

        def agp_copy(r, k):
            return remote(own_piece(r, k), y_at(r, chip, k), agp_send.at[k], p_recv.at[group(r)], partner)

        def fw_copy(r, k, s):
            q = (left_chip, right_chip)[s]
            return remote(y_at(r, q, k, s), y_at(r, q, k, s), fw_send.at[s, k], fw_recv.at[s, k], sides[s])

        def p_copy(r, k, q):
            return remote(y_at(r, q, k), y_at(r, q, k), p_send.at[group(r)], p_recv.at[group(r)], partner)

        def first_sends(r, k):
            for s in range(2):
                rly_copy(r, k, s).start()
            for s in range(2):
                dir_copy(r, k, s).start()

        def stage1(r, k):
            for s in range(2):
                rly_copy(r, k, s).wait_recv()
                rr = rows_of(r, (right_chip, left_chip)[s], s)
                sb[k, rr] = (sb[k, rr].astype(F32) + rly[s, k, pl.ds(0, size[r] // parts)].astype(F32)).astype(BF16)
            for s in range(2):
                rel_copy(r, k, s).start()

        def stage2(r, k):
            for s in range(2):
                rly_copy(r, k, s).wait_send()
                dir_copy(r, k, s).wait()
                rel_copy(r, k, s).wait_recv()
            at = pl.ds(0, size[r] // parts)
            for part in range(2):
                rr = rows_of(r, chip, part)
                from_left = (relb if part == 0 else dirb)[0, k, at].astype(F32)
                from_right = (relb if part == 1 else dirb)[1, k, at].astype(F32)
                sb[k, rr] = (sb[k, rr].astype(F32) + from_left + from_right).astype(BF16)
            for s in range(2):
                ag_copy(r, k, s).start()
            agp_copy(r, k).start()
            loc_copy(r, k).start()

        def stage3(r, k):
            for s in range(2):
                rel_copy(r, k, s).wait_send()
                ag_copy(r, k, s).wait_recv()
            for s in range(2):
                fw_copy(r, k, s).start()
            p_copy(r, k, left_chip).start()
            p_copy(r, k, right_chip).start()
            loc_copy(r, k).wait()

        def stage4(r, k):
            for s in range(2):
                ag_copy(r, k, s).wait_send()
                fw_copy(r, k, s).wait()
            agp_copy(r, k).wait_send()
            p_copy(r, k, far_chip).start()

        def events(j, r):
            @pl.when(j < 2)
            def _():
                stage1(r, j + 3)

            @pl.when(jnp.logical_and(j >= 1, j < 5))
            def _():
                stage2(r, j)

            @pl.when(jnp.logical_and(j >= 2, j < 7))
            def _():
                stage3(r, j - 2)

            @pl.when(j >= 5)
            def _():
                stage4(r, j - 5)

            @pl.when(j == 8)
            def _():
                stage4(r, 4)

        x_copy(0).start()
        for c in gu_copies(0, 0):
            c.start()
        barrier = pltpu.get_barrier_semaphore()
        for to in (right, left, partner):
            pl.semaphore_signal(barrier, inc=1, device_id={"tp": to}, device_id_type=MESH)
        pl.semaphore_wait(barrier, 3)
        for k in range(nd):
            wd_copy(k).start()

        def start_down(r, k):
            if r == 0:
                wd_copy(k).wait_recv()
            for c in d_copies(k, lax.rem(k, 2)):
                c.start()

        for r in range(nr):
            x_copy(r).wait()
            all_rows = pl.ds(0, size[r])

            def gate_up(j, _):
                slot = lax.rem(r * ng + j, 2)
                for c in gu_copies(j, slot):
                    c.wait()
                if r == 0:
                    @pl.when(j == 0)
                    def _():
                        for c in gu_copies(1, 1):
                            c.start()
                acc = jnp.dot(xb[all_rows], wgu[slot], preferred_element_type=F32)
                gate, up = acc[:, :gb], acc[:, gb:]
                hid[all_rows, ds(j * gb, gb, 128)] = (jax.nn.silu(gate) * up).astype(BF16)

                def refill():
                    for c in gu_copies(lax.rem(j + 2, ng), slot):
                        c.start()
                if r < nr - 1:
                    refill()
                else:
                    pl.when(j < ng - 2)(refill)
                if r > 0:
                    @pl.when(j == 0)
                    def _():
                        pl.semaphore_wait(credit, 1)
                h_copy(r, j).start()

                @pl.when(j == 3)
                def _():
                    start_down(r, 0)

                @pl.when(j == 5)
                def _():
                    start_down(r, 1)
                if r > 0:
                    events(j, r - 1)
                return 0

            lax.fori_loop(0, ng, gate_up, 0)
            if r < nr - 1:
                x_copy(r + 1).start()

            h_all(r).wait()

            def down(k, _):
                slot = lax.rem(k, 2)
                for c in d_copies(k, slot):
                    c.wait()
                acc = jnp.dot(hid[all_rows], wdb[slot], preferred_element_type=F32)
                sb[k, all_rows] = acc.astype(BF16)

                @pl.when(k < nd - 2)
                def _():
                    start_down(r, k + 2)
                first_sends(r, k)

                @pl.when(k >= 2)
                def _():
                    stage1(r, k - 2)

                @pl.when(k == nd - 1)
                def _():
                    stage2(r, 0)
                return 0

            lax.fori_loop(0, nd, down, 0)
            if r < nr - 1:
                pl.semaphore_signal(credit, inc=1, device_id={"tp": partner}, device_id_type=MESH)

        def wait_partner(i, ref):
            n_rows = ref.shape[0]
            sent = ref.at[pl.ds(0, n_rows - n_rows // chips), ds(my_half, half, 128)]
            came = ref.at[:, ds(partner_half, half, 128)]
            remote(sent, sent, p_send.at[i], p_recv.at[i], partner).wait_send()
            remote(came, came, p_send.at[i], p_recv.at[i], partner).wait_recv()

        wait_partner(0, early_ref)
        early_copy = pltpu.make_async_copy(early_ref, hid.at[:, pl.ds(0, d)], x_sem)
        early_copy.start()

        def tail(j, _):
            events(j, nr - 1)
            return 0

        lax.fori_loop(0, ng, tail, 0)
        for k in range(nd):
            wd_copy(k).wait_send()
        wait_partner(1, mid_ref)
        wait_partner(2, xb)
        early_copy.wait()

    dma = pltpu.SemaphoreType.DMA
    first, middle, last, _, _ = pl.pallas_call(
        kernel,
        out_shape=(pltpu.VMEM((top, CORES * f), BF16), pltpu.VMEM((base[-1] - base[1], d), BF16), pltpu.VMEM((top, d), BF16),
                   pltpu.HBM((size[0], d), BF16), pltpu.HBM((f, half), BF16)),
        in_specs=[pl.BlockSpec(memory_space=pl.ANY)] * 4,
        out_specs=tuple(pl.BlockSpec(memory_space=m) for m in (pltpu.VMEM,) * 3 + (pltpu.HBM,) * 2),
        scratch_shapes=[
            pltpu.VMEM((2, d, 2 * gb), BF16),
            pltpu.VMEM((2, CORES * f, db), BF16),
            pltpu.VMEM((nd, top, db), BF16),
            pltpu.VMEM((2, nd, top // parts, db), BF16),
            pltpu.VMEM((2, nd, top // parts, db), BF16),
            pltpu.VMEM((2, nd, top // parts, db), BF16),
            dma, dma((2, 2)), dma((2, 2)),
            dma((nd,)), dma((nd,)), dma, dma, pltpu.SemaphoreType.REGULAR,
            dma((2, nd)), dma((2, nd)), dma((2, nd)), dma((2, nd)), dma((2, nd)), dma((2, nd)),
            dma((2, nd)), dma((2, nd)), dma((nd,)), dma((2, nd)), dma((2, nd)), dma((nd,)), dma((3,)), dma((3,)),
        ],
        compiler_params=pltpu.CompilerParams(
            collective_id=0, has_side_effects=True, vmem_limit_bytes=KERNEL_VMEM),
        cost_estimate=pl.CostEstimate(flops=6 * rows * d * f, bytes_accessed=2 * 3 * d * f * nr, transcendentals=rows * f),
        name="mlp_block",
    )(x, w_gate, w_up, w_down)
    return join(d, first, middle, last)


def solution(mesh):
    return jax.shard_map(
        functools.partial(block, mesh.shape["tp"]),
        mesh=mesh,
        in_specs=(P("dp", None), P(None, "tp"), P(None, "tp"), P("tp", None)),
        out_specs=P("dp", None),
        check_vma=False,
    )
```
